32 devices in a mesh: blk: 16 (over z, y, x), grp: 2 (over core).
Axes of the slice: x: 2, y: 2, z: 4, core: 2. Of those that a mesh axis runs over, the one named last changes fastest.
Arguments:
- text: bfloat16 [16, 384, 1024], P('blk', 'grp'), may hold values from -64 to 64
- image: bfloat16 [16, 384, 1024], P('blk', 'grp'), may hold values from -64 to 64
- pair_index: int32 [16, 384], P('blk', 'grp'), may hold values from 0 to 383, each once within a row
Outputs:
- grad_text: float32 [16, 384, 1024], P('blk', 'grp')
- grad_image: float32 [16, 384, 1024], P('blk', 'grp')
- loss: float32 [], replicated
The draws below stay inside these ranges and needn't reach their ends.
Inputs may be any that keep to these rules, and one draw needn't show every extreme that they name: Every sub-batch's row of pair_index names each of 0 to 383 once.
All inputs are finite; a program needn't handle non-finite values.
Results may differ from the reference program's by a relative error of at most 0.0024.
Values may be sent and summed in bfloat16 or wider, within the bound.
A program may use at most 64 MiB of HBM per device.

```python
import jax
import jax.numpy as jnp

D = 1024
SUB = 384
GROUPS = 16


def embed_pair(key):
    key = jax.random.fold_in(key, 7)
    keys = jax.random.split(key, 6)
    text_base = jax.random.normal(keys[0], (GROUPS, SUB, D), jnp.float32)
    image_base = jax.random.normal(keys[1], (GROUPS, SUB, D), jnp.float32)
    text_out = text_base
    image_out = image_base
    targets = (110.0, 150.0, 200.0, 260.0)
    for number in range(4):
        target = targets[number]
        first_row = number * (SUB // 4)
        base = image_base[:, first_row + 1]
        noise_a = jax.random.normal(jax.random.fold_in(keys[4], number), (GROUPS, D), jnp.float32)
        noise_b = jax.random.normal(jax.random.fold_in(keys[5], number), (GROUPS, D), jnp.float32)
        base_sq = jnp.sum(base * base, axis=-1, keepdims=True)
        perp_a = noise_a - jnp.sum(noise_a * base, axis=-1, keepdims=True) / base_sq * base
        perp_b = noise_b - jnp.sum(noise_b * base, axis=-1, keepdims=True) / base_sq * base
        stretch = jnp.sqrt(target / (0.125 * base_sq))
        aligned = stretch * base
        shrink = 1.0 - 2.0 / target
        image_out = image_out.at[:, first_row + 1].set(aligned)
        image_out = image_out.at[:, first_row + 2].set(shrink * aligned + perp_a)
        text_out = text_out.at[:, first_row].set(aligned)
        text_out = text_out.at[:, first_row + 1].set(shrink * aligned + perp_b)
    return (jnp.clip(text_out, -64.0, 64.0), jnp.clip(image_out, -64.0, 64.0))


def draw_text(key, part):
    return embed_pair(key)[0].astype(jnp.bfloat16)


def draw_image(key, part):
    return embed_pair(key)[1].astype(jnp.bfloat16)


def setup_inputs(seed: int = 0) -> dict:
    key_of = jax.random.split(jax.random.key(seed), 4)
    return {
        "text": draw_text(jax.random.fold_in(key_of[3], 71), 0),
        "image": draw_image(jax.random.fold_in(key_of[3], 71), 0),
        "pair_index": jax.vmap(lambda own: jax.random.permutation(own, SUB))(jax.random.split(key_of[2], GROUPS)).reshape((GROUPS, SUB)).astype(jnp.int32),
    }


score_scale = 0.125


def group_terms(text_rows, image_rows, pairs):
    scores = jnp.dot(text_rows, image_rows.T, preferred_element_type=jnp.float32) * score_scale
    row_top = jnp.max(scores, axis=1)
    row_lse = row_top + jnp.log(jnp.sum(jnp.exp(scores - row_top[:, None]), axis=1))
    col_top = jnp.max(scores, axis=0)
    col_lse = col_top + jnp.log(jnp.sum(jnp.exp(scores - col_top[None, :]), axis=0))
    hit = pairs[:, None] == jnp.arange(SUB, dtype=jnp.int32)[None, :]
    positive = jnp.sum(jnp.where(hit, scores, 0.0), axis=1)
    weight = (jnp.exp(scores - row_lse[:, None]) + jnp.exp(scores - col_lse[None, :]) - 2.0 * hit.astype(jnp.float32)).astype(jnp.bfloat16)
    grad_t = jnp.dot(weight, image_rows, preferred_element_type=jnp.float32) * (score_scale * 0.5)
    grad_i = jnp.dot(weight.T, text_rows, preferred_element_type=jnp.float32) * (score_scale * 0.5)
    partial_sum = jnp.sum(row_lse - 2.0 * positive) + jnp.sum(col_lse)
    return grad_t, grad_i, partial_sum


def reference(text, image, pair_index):
    grads_t = []
    grads_i = []
    total = jnp.zeros((), jnp.float32)
    for group in range(GROUPS):
        grad_t, grad_i, partial_sum = group_terms(text[group], image[group], pair_index[group])
        grads_t.append(grad_t)
        grads_i.append(grad_i)
        total = total + partial_sum
    loss = total / (2.0 * SUB * GROUPS)
    return jnp.stack(grads_t), jnp.stack(grads_i), loss
```

```python
import functools

import jax
import jax.numpy as jnp
from jax import lax
from jax.experimental import pallas as pl
from jax.experimental.pallas import tpu as pltpu
from jax.sharding import PartitionSpec as P

score_scale = 0.125
MESH = pl.DeviceIdType.MESH
F32 = jnp.float32


def loop(start, stop, body):
    if stop - start <= 16:
        for number in range(start, stop):
            body(number)
    else:
        pl.loop(start, stop)(body)


def kernel(
    groups,
    blocks,
    text_in,
    image_in,
    pairs_in,
    grad_text,
    grad_image,
    loss,
    text,
    image,
    pairs,
    scores,
    row_exp,
    col_exp,
    row_scale,
    col_scale,
    columns,
    parts,
    out_text,
    out_image,
    load_sem,
    send_sem,
    recv_sem,
    loss_send,
    loss_recv,
    store_sem,
):
    blk = lax.axis_index("blk")
    me = lax.axis_index("grp")
    rows = text_in.shape[1]

    loads = [
        pltpu.make_async_copy(source.at[0], target.at[me], load_sem.at[number])
        for number, (source, target) in enumerate(((image_in, image), (text_in, text)))
    ]
    loads.append(pltpu.make_async_copy(pairs_in, pairs.at[me], load_sem.at[2]))
    for load in loads:
        load.start()

    barrier = pltpu.get_barrier_semaphore()

    def greet_group(step):
        peer = lax.rem(me + step, groups)
        pl.semaphore_signal(barrier, inc=1, device_id={"grp": peer}, device_id_type=MESH)

    def greet_block(step):
        peer = lax.rem(blk + step, blocks)
        pl.semaphore_signal(barrier, inc=1, device_id={"blk": peer}, device_id_type=MESH)

    loop(1, groups, greet_group)
    loop(1, blocks, greet_block)

    def send(kind, buffer, step):
        peer = lax.rem(me + step, groups)
        return pltpu.make_async_remote_copy(
            src_ref=buffer.at[me],
            dst_ref=buffer.at[me],
            send_sem=send_sem.at[kind, step],
            recv_sem=recv_sem.at[kind, step],
            device_id={"grp": peer},
            device_id_type=MESH,
        )

    def arrive(kind, buffer, step):
        source = lax.rem(me - step + groups, groups)
        pltpu.make_async_remote_copy(
            src_ref=buffer.at[source],
            dst_ref=buffer.at[source],
            send_sem=send_sem.at[kind, step],
            recv_sem=recv_sem.at[kind, step],
            device_id={"grp": source},
            device_id_type=MESH,
        ).wait_recv()
        return source

    for load in loads:
        load.wait()
    pl.semaphore_wait(barrier, groups - 1 + blocks - 1)

    buffers = (image, text, pairs)
    for kind, buffer in ((2, pairs), (0, image), (1, text)):
        loop(1, groups, lambda step, kind=kind, buffer=buffer: send(kind, buffer, step).start())

    def score(t, i):
        scores[t, i] = (
            lax.dot_general(
                text[t], image[i], (((1,), (1,)), ((), ())), preferred_element_type=F32
            )
            * score_scale
        )

    score(me, me)

    def pair_step(step):
        arrive(2, pairs, step)

    loop(1, groups, pair_step)
    same = lax.broadcasted_iota(jnp.int32, (rows, rows), 0) == lax.broadcasted_iota(
        jnp.int32, (rows, rows), 1
    )

    def column_step(t):
        values = jnp.broadcast_to(pairs[t].astype(F32), (rows, rows))
        columns[t] = jnp.sum(jnp.where(same, values, 0.0), axis=1, keepdims=True)

    loop(0, groups, column_step)

    def image_step(step):
        score(me, arrive(0, image, step))

    def text_step(step):
        t = arrive(1, text, step)
        loop(0, groups, lambda i: score(t, i))

    loop(1, groups, image_step)
    loop(1, groups, text_step)

    lane = lax.broadcasted_iota(jnp.int32, (rows, rows), 1)

    def hits(t, i):
        return columns[t] == (lane + i * rows).astype(F32)

    def over(count, first, join, value):
        if count <= 8:
            total = first
            for number in range(count):
                total = join(total, value(number))
            return total
        return lax.fori_loop(0, count, lambda n, total: join(total, value(n)), first)

    add = lambda left, right: left + right
    low = -jnp.inf

    def row_step(t, total):
        top = over(
            groups,
            jnp.full((rows, 1), low, F32),
            jnp.maximum,
            lambda i: jnp.max(scores[t, i], axis=1, keepdims=True),
        )

        def term(i):
            value = jnp.exp(scores[t, i] - top)
            row_exp[t, i] = value
            return jnp.sum(value, axis=1, keepdims=True)

        amount = over(groups, jnp.zeros((rows, 1), F32), add, term)
        row_scale[t] = 1.0 / amount
        hit_sum = over(
            groups,
            jnp.zeros((1, rows), F32),
            add,
            lambda i: jnp.sum(jnp.where(hits(t, i), scores[t, i], 0.0), axis=0, keepdims=True),
        )
        return (
            total
            + jnp.sum(top + jnp.log(amount), keepdims=True)
            - 2.0 * jnp.sum(hit_sum, axis=1, keepdims=True)
        )

    def col_step(i, total):
        top = over(
            groups,
            jnp.full((1, rows), low, F32),
            jnp.maximum,
            lambda t: jnp.max(scores[t, i], axis=0, keepdims=True),
        )

        def term(t):
            value = jnp.exp(scores[t, i] - top)
            col_exp[t, i] = value
            return jnp.sum(value, axis=0, keepdims=True)

        amount = over(groups, jnp.zeros((1, rows), F32), add, term)
        col_scale[i] = 1.0 / amount
        return total + jnp.sum(top + jnp.log(amount), axis=1, keepdims=True)

    total = jnp.zeros((1, 1), F32)
    for number in range(groups):
        total = row_step(number, total)
    for number in range(groups):
        total = col_step(number, total)
    parts[blk] = jnp.broadcast_to(total, (1, 128))

    def tell(step):
        peer = lax.rem(blk + step, blocks)
        return pltpu.make_async_remote_copy(
            src_ref=parts.at[blk],
            dst_ref=parts.at[blk],
            send_sem=loss_send.at[step],
            recv_sem=loss_recv.at[step],
            device_id={"blk": peer},
            device_id_type=MESH,
        )

    def hear(step):
        source = lax.rem(blk - step + blocks, blocks)
        pltpu.make_async_remote_copy(
            src_ref=parts.at[source],
            dst_ref=parts.at[source],
            send_sem=loss_send.at[step],
            recv_sem=loss_recv.at[step],
            device_id={"blk": source},
            device_id_type=MESH,
        ).wait_recv()

    loop(1, blocks, lambda step: tell(step).start())

    def weight(t, i):
        return (
            row_exp[t, i] * row_scale[t]
            + col_exp[t, i] * col_scale[i]
            - jnp.where(hits(t, i), 2.0, 0.0)
        ).astype(jnp.bfloat16)

    half = score_scale * 0.5
    grad = jnp.zeros((rows, text_in.shape[2]), F32)
    out_text[...] = (
        over(
            groups,
            grad,
            add,
            lambda i: jnp.dot(weight(me, i), image[i], preferred_element_type=F32),
        )
        * half
    )
    store_text = pltpu.make_async_copy(out_text, grad_text.at[0], store_sem.at[0])
    store_text.start()
    out_image[...] = (
        over(
            groups,
            grad,
            add,
            lambda t: lax.dot_general(
                weight(t, me), text[t], (((0,), (0,)), ((), ())), preferred_element_type=F32
            ),
        )
        * half
    )
    store_image = pltpu.make_async_copy(out_image, grad_image.at[0], store_sem.at[1])
    store_image.start()

    for kind, buffer in enumerate(buffers):
        loop(
            1, groups, lambda step, kind=kind, buffer=buffer: send(kind, buffer, step).wait_send()
        )
    loop(1, blocks, lambda step: tell(step).wait_send())
    loop(1, blocks, hear)
    whole = jnp.sum(parts[...].reshape(blocks, 128), axis=0, keepdims=True)
    loss[...] = whole[:, 0:1] / (2.0 * rows * groups * blocks)
    store_text.wait()
    store_image.wait()


def solution(mesh):
    groups, blocks = mesh.shape["grp"], mesh.shape["blk"]

    def local(text, image, pair_index):
        _, rows, width = text.shape
        anywhere = pl.BlockSpec(memory_space=pl.ANY)
        square = pltpu.VMEM((groups, groups, rows, rows), F32)
        grads_t, grads_i, loss = pl.pallas_call(
            functools.partial(kernel, groups, blocks),
            out_shape=(
                jax.ShapeDtypeStruct(text.shape, F32),
                jax.ShapeDtypeStruct(image.shape, F32),
                jax.ShapeDtypeStruct((1, 1), F32),
            ),
            in_specs=[anywhere] * 3,
            out_specs=(anywhere, anywhere, pl.BlockSpec(memory_space=pltpu.VMEM)),
            scratch_shapes=[
                pltpu.VMEM((groups, rows, width), text.dtype),
                pltpu.VMEM((groups, rows, width), image.dtype),
                pltpu.VMEM((groups, 1, rows), jnp.int32),
                square,
                square,
                square,
                pltpu.VMEM((groups, rows, 1), F32),
                pltpu.VMEM((groups, 1, rows), F32),
                pltpu.VMEM((groups, rows, 1), F32),
                pltpu.VMEM((blocks, 1, 128), F32),
                pltpu.VMEM((rows, width), F32),
                pltpu.VMEM((rows, width), F32),
                pltpu.SemaphoreType.DMA((3,)),
                pltpu.SemaphoreType.DMA((3, groups)),
                pltpu.SemaphoreType.DMA((3, groups)),
                pltpu.SemaphoreType.DMA((blocks,)),
                pltpu.SemaphoreType.DMA((blocks,)),
                pltpu.SemaphoreType.DMA((2,)),
            ],
            compiler_params=pltpu.CompilerParams(collective_id=0, has_side_effects=True),
        )(text, image, pair_index)
        return grads_t, grads_i, loss.reshape(())

    placed = (P("blk", "grp", None), P("blk", "grp", None), P("blk", "grp"))
    return jax.shard_map(
        local,
        mesh=mesh,
        in_specs=placed,
        out_specs=(P("blk", "grp", None), P("blk", "grp", None), P()),
        check_vma=False,
    )
```

```python
import functools

import jax
import jax.numpy as jnp
from jax import lax
from jax.experimental import pallas as pl
from jax.experimental.pallas import tpu as pltpu
from jax.sharding import PartitionSpec as P

score_scale = 0.125
MESH = pl.DeviceIdType.MESH
F32 = jnp.float32


def loop(start, stop, body):
    if stop - start <= 16:
        for number in range(start, stop):
            body(number)
    else:
        pl.loop(start, stop)(body)


def kernel(
    groups,
    blocks,
    text_in,
    image_in,
    pairs_in,
    grad_text,
    grad_image,
    loss,
    text,
    image,
    pairs,
    scores,
    row_exp,
    col_exp,
    row_scale,
    col_scale,
    columns,
    parts,
    out_text,
    out_image,
    load_sem,
    send_sem,
    recv_sem,
    loss_send,
    loss_recv,
    store_sem,
    ready,
):
    blk = lax.axis_index("blk")
    me = lax.axis_index("grp")
    rows = text_in.shape[1]

    loads = [
        pltpu.make_async_copy(source.at[0], target.at[me], load_sem.at[number])
        for number, (source, target) in enumerate(((image_in, image), (text_in, text)))
    ]
    loads.append(pltpu.make_async_copy(pairs_in, pairs.at[me], load_sem.at[2]))
    for load in loads:
        load.start()

    barrier = pltpu.get_barrier_semaphore()
    sender = me == 0

    def greet_group(peer):
        pl.semaphore_signal(barrier, inc=1, device_id={"grp": peer}, device_id_type=MESH)

    def greet_block(step):
        pl.semaphore_signal(
            barrier,
            inc=1,
            device_id={"blk": lax.rem(blk + step, blocks), "grp": 0},
            device_id_type=MESH,
        )

    @pl.when(sender)
    def _():
        loop(1, groups, greet_group)

    @pl.when(jnp.logical_not(sender))
    def _():
        pl.semaphore_wait(barrier, 1)
        pl.semaphore_signal(ready, inc=1, device_id={"grp": 0}, device_id_type=MESH)

    loop(1, blocks, greet_block)

    @pl.when(sender)
    def _():
        pl.semaphore_wait(ready, groups - 1)
        if groups > 2:

            def allow(peer):
                pl.semaphore_signal(ready, inc=1, device_id={"grp": peer}, device_id_type=MESH)

            loop(1, groups, allow)

    if groups > 2:

        @pl.when(jnp.logical_not(sender))
        def _():
            pl.semaphore_wait(ready, 1)

    def send(kind, buffer, step):
        peer = lax.rem(me + step, groups)
        return pltpu.make_async_remote_copy(
            src_ref=buffer.at[me],
            dst_ref=buffer.at[me],
            send_sem=send_sem.at[kind, step],
            recv_sem=recv_sem.at[kind, step],
            device_id={"grp": peer},
            device_id_type=MESH,
        )

    def arrive(kind, buffer, step):
        source = lax.rem(me - step + groups, groups)
        pltpu.make_async_remote_copy(
            src_ref=buffer.at[source],
            dst_ref=buffer.at[source],
            send_sem=send_sem.at[kind, step],
            recv_sem=recv_sem.at[kind, step],
            device_id={"grp": source},
            device_id_type=MESH,
        ).wait_recv()
        return source

    buffers = (image, text, pairs)
    for kind, buffer in ((2, pairs), (0, image), (1, text)):
        loads[kind].wait()
        loop(1, groups, lambda step, kind=kind, buffer=buffer: send(kind, buffer, step).start())

    def score(t, i):
        scores[t, i] = (
            lax.dot_general(
                text[t], image[i], (((1,), (1,)), ((), ())), preferred_element_type=F32
            )
            * score_scale
        )

    score(me, me)

    def pair_step(step):
        arrive(2, pairs, step)

    loop(1, groups, pair_step)
    same = lax.broadcasted_iota(jnp.int32, (rows, rows), 0) == lax.broadcasted_iota(
        jnp.int32, (rows, rows), 1
    )

    def column_step(t):
        values = jnp.broadcast_to(pairs[t].astype(F32), (rows, rows))
        columns[t] = jnp.sum(jnp.where(same, values, 0.0), axis=1, keepdims=True)

    loop(0, groups, column_step)

    def image_step(step):
        score(me, arrive(0, image, step))

    def text_step(step):
        t = arrive(1, text, step)
        loop(0, groups, lambda i: score(t, i))

    loop(1, groups, image_step)
    loop(1, groups, text_step)

    lane = lax.broadcasted_iota(jnp.int32, (rows, rows), 1)

    def hits(t, i):
        return columns[t] == (lane + i * rows).astype(F32)

    def over(count, first, join, value):
        if count <= 8:
            total = first
            for number in range(count):
                total = join(total, value(number))
            return total
        return lax.fori_loop(0, count, lambda n, total: join(total, value(n)), first)

    add = lambda left, right: left + right
    low = -jnp.inf

    def row_step(t, total):
        top = over(
            groups,
            jnp.full((rows, 1), low, F32),
            jnp.maximum,
            lambda i: jnp.max(scores[t, i], axis=1, keepdims=True),
        )

        def term(i):
            value = jnp.exp(scores[t, i] - top)
            row_exp[t, i] = value
            return jnp.sum(value, axis=1, keepdims=True)

        amount = over(groups, jnp.zeros((rows, 1), F32), add, term)
        row_scale[t] = 1.0 / amount
        hit_sum = over(
            groups,
            jnp.zeros((1, rows), F32),
            add,
            lambda i: jnp.sum(jnp.where(hits(t, i), scores[t, i], 0.0), axis=0, keepdims=True),
        )
        return (
            total
            + jnp.sum(top + jnp.log(amount), keepdims=True)
            - 2.0 * jnp.sum(hit_sum, axis=1, keepdims=True)
        )

    def col_step(i, total):
        top = over(
            groups,
            jnp.full((1, rows), low, F32),
            jnp.maximum,
            lambda t: jnp.max(scores[t, i], axis=0, keepdims=True),
        )

        def term(t):
            value = jnp.exp(scores[t, i] - top)
            col_exp[t, i] = value
            return jnp.sum(value, axis=0, keepdims=True)

        amount = over(groups, jnp.zeros((1, rows), F32), add, term)
        col_scale[i] = 1.0 / amount
        return total + jnp.sum(top + jnp.log(amount), axis=1, keepdims=True)

    total = jnp.zeros((1, 1), F32)
    for number in range(groups):
        total = row_step(number, total)
    for number in range(groups):
        total = col_step(number, total)
    parts[blk] = jnp.broadcast_to(total, (1, 128))

    def tell(step, peer):
        return pltpu.make_async_remote_copy(
            src_ref=parts.at[blk],
            dst_ref=parts.at[blk],
            send_sem=loss_send.at[step, peer],
            recv_sem=loss_recv.at[step],
            device_id={"blk": lax.rem(blk + step, blocks), "grp": peer},
            device_id_type=MESH,
        )

    def hear(step):
        source = lax.rem(blk - step + blocks, blocks)
        pltpu.make_async_remote_copy(
            src_ref=parts.at[source],
            dst_ref=parts.at[source],
            send_sem=loss_send.at[step, 0],
            recv_sem=loss_recv.at[step],
            device_id={"blk": source, "grp": 0},
            device_id_type=MESH,
        ).wait_recv()

    @pl.when(sender)
    def _():
        pl.semaphore_wait(barrier, (blocks - 1) * groups)
        loop(1, blocks, lambda step: loop(0, groups, lambda peer: tell(step, peer).start()))

    def weight(t, i):
        return (
            row_exp[t, i] * row_scale[t]
            + col_exp[t, i] * col_scale[i]
            - jnp.where(hits(t, i), 2.0, 0.0)
        ).astype(jnp.bfloat16)

    half = score_scale * 0.5
    grad = jnp.zeros((rows, text_in.shape[2]), F32)
    out_text[...] = (
        over(
            groups,
            grad,
            add,
            lambda i: jnp.dot(weight(me, i), image[i], preferred_element_type=F32),
        )
        * half
    )
    store_text = pltpu.make_async_copy(out_text, grad_text.at[0], store_sem.at[0])
    store_text.start()
    out_image[...] = (
        over(
            groups,
            grad,
            add,
            lambda t: lax.dot_general(
                weight(t, me), text[t], (((0,), (0,)), ((), ())), preferred_element_type=F32
            ),
        )
        * half
    )
    store_image = pltpu.make_async_copy(out_image, grad_image.at[0], store_sem.at[1])
    store_image.start()

    for kind, buffer in enumerate(buffers):
        loop(
            1, groups, lambda step, kind=kind, buffer=buffer: send(kind, buffer, step).wait_send()
        )

    @pl.when(sender)
    def _():
        loop(1, blocks, lambda step: loop(0, groups, lambda peer: tell(step, peer).wait_send()))

    loop(1, blocks, hear)
    whole = jnp.sum(parts[...].reshape(blocks, 128), axis=0, keepdims=True)
    loss[...] = whole[:, 0:1] / (2.0 * rows * groups * blocks)
    store_text.wait()
    store_image.wait()


def solution(mesh):
    groups, blocks = mesh.shape["grp"], mesh.shape["blk"]

    def local(text, image, pair_index):
        _, rows, width = text.shape
        anywhere = pl.BlockSpec(memory_space=pl.ANY)
        square = pltpu.VMEM((groups, groups, rows, rows), F32)
        grads_t, grads_i, loss = pl.pallas_call(
            functools.partial(kernel, groups, blocks),
            out_shape=(
                jax.ShapeDtypeStruct(text.shape, F32),
                jax.ShapeDtypeStruct(image.shape, F32),
                jax.ShapeDtypeStruct((1, 1), F32),
            ),
            in_specs=[pl.BlockSpec(memory_space=pltpu.HBM)] * 3,
            out_specs=(anywhere, anywhere, pl.BlockSpec(memory_space=pltpu.VMEM)),
            scratch_shapes=[
                pltpu.VMEM((groups, rows, width), text.dtype),
                pltpu.VMEM((groups, rows, width), image.dtype),
                pltpu.VMEM((groups, 1, rows), jnp.int32),
                square,
                square,
                square,
                pltpu.VMEM((groups, rows, 1), F32),
                pltpu.VMEM((groups, 1, rows), F32),
                pltpu.VMEM((groups, rows, 1), F32),
                pltpu.VMEM((blocks, 1, 128), F32),
                pltpu.VMEM((rows, width), F32),
                pltpu.VMEM((rows, width), F32),
                pltpu.SemaphoreType.DMA((3,)),
                pltpu.SemaphoreType.DMA((3, groups)),
                pltpu.SemaphoreType.DMA((3, groups)),
                pltpu.SemaphoreType.DMA((blocks, groups)),
                pltpu.SemaphoreType.DMA((blocks,)),
                pltpu.SemaphoreType.DMA((2,)),
                pltpu.SemaphoreType.REGULAR,
            ],
            compiler_params=pltpu.CompilerParams(collective_id=0, has_side_effects=True, vmem_limit_bytes=40 << 20),
        )(*(pltpu.with_memory_space_constraint(x, pltpu.HBM) for x in (text, image, pair_index)))
        return grads_t, grads_i, loss.reshape(())

    placed = (P("blk", "grp", None), P("blk", "grp", None), P("blk", "grp"))
    return jax.shard_map(
        local,
        mesh=mesh,
        in_specs=placed,
        out_specs=(P("blk", "grp", None), P("blk", "grp", None), P()),
        check_vma=False,
    )
```

```python
import functools

import jax
import jax.numpy as jnp
from jax import lax
from jax.experimental import pallas as pl
from jax.experimental.pallas import tpu as pltpu
from jax.sharding import PartitionSpec as P

score_scale = 0.125
MESH = pl.DeviceIdType.MESH
F32 = jnp.float32


def loop(start, stop, body):
    if stop - start <= 16:
        for number in range(start, stop):
            body(number)
    else:
        pl.loop(start, stop)(body)


def kernel(
    groups,
    blocks,
    text_in,
    image_in,
    pairs_in,
    grad_text,
    grad_image,
    loss,
    text,
    image,
    pairs,
    scores,
    row_exp,
    col_exp,
    row_scale,
    col_scale,
    columns,
    parts,
    out_text,
    out_image,
    load_sem,
    send_sem,
    recv_sem,
    loss_send,
    loss_recv,
    store_sem,
    ready,
    terms,
):
    blk = lax.axis_index("blk")
    me = lax.axis_index("grp")
    rows = text_in.shape[1]

    pieces = 4 if rows % 64 == 0 else 1
    step_rows = rows // pieces
    strips = [pl.ds(piece * step_rows, step_rows) for piece in range(pieces)]

    barrier = pltpu.get_barrier_semaphore()
    sender = me == 0

    loads = [
        [
            pltpu.make_async_copy(
                source.at[0, strip], target.at[me, strip], load_sem.at[kind, piece]
            )
            for piece, strip in enumerate(strips)
        ]
        for kind, (source, target) in enumerate(((image_in, image), (text_in, text)))
    ]
    loads.append([pltpu.make_async_copy(pairs_in, pairs.at[me], load_sem.at[2, 0])])

    def greet_group(peer):
        pl.semaphore_signal(barrier, inc=1, device_id={"grp": peer}, device_id_type=MESH)

    def greet_block(step):
        pl.semaphore_signal(
            barrier,
            inc=1,
            device_id={"blk": lax.rem(blk + step, blocks), "grp": 0},
            device_id_type=MESH,
        )

    @pl.when(sender)
    def _():
        loop(1, groups, greet_group)

    for load in loads[2] + loads[0] + loads[1]:
        load.start()

    @pl.when(jnp.logical_not(sender))
    def _():
        pl.semaphore_wait(barrier, 1)
        pl.semaphore_signal(ready, inc=1, device_id={"grp": 0}, device_id_type=MESH)

    loop(1, blocks, greet_block)

    @pl.when(sender)
    def _():
        pl.semaphore_wait(ready, groups - 1)
        if groups > 2:

            def allow(peer):
                pl.semaphore_signal(ready, inc=1, device_id={"grp": peer}, device_id_type=MESH)

            loop(1, groups, allow)

    if groups > 2:

        @pl.when(jnp.logical_not(sender))
        def _():
            pl.semaphore_wait(ready, 1)

    def views(kind, buffer, owner):
        if kind == 2:
            return [buffer.at[owner]]
        return [buffer.at[owner, strip] for strip in strips]

    def swap(kind, buffer, owner, step, peer, piece):
        view = views(kind, buffer, owner)[piece]
        return pltpu.make_async_remote_copy(
            src_ref=view,
            dst_ref=view,
            send_sem=send_sem.at[kind, step, piece],
            recv_sem=recv_sem.at[kind, step, piece],
            device_id={"grp": peer},
            device_id_type=MESH,
        )

    def send(kind, buffer, step, piece):
        return swap(kind, buffer, me, step, lax.rem(me + step, groups), piece)

    def arrive(kind, buffer, step):
        source = lax.rem(me - step + groups, groups)
        for piece in range(len(loads[kind])):
            swap(kind, buffer, source, step, source, piece).wait_recv()
        return source

    buffers = (image, text, pairs)
    for kind, buffer in ((2, pairs), (0, image), (1, text)):
        for piece, load in enumerate(loads[kind]):
            load.wait()
            loop(
                1,
                groups,
                lambda step, kind=kind, buffer=buffer, piece=piece: send(
                    kind, buffer, step, piece
                ).start(),
            )

    def score(t, i):
        scores[t, i] = (
            lax.dot_general(
                text[t], image[i], (((1,), (1,)), ((), ())), preferred_element_type=F32
            )
            * score_scale
        )

    score(me, me)

    def pair_step(step):
        arrive(2, pairs, step)

    loop(1, groups, pair_step)
    same = lax.broadcasted_iota(jnp.int32, (rows, rows), 0) == lax.broadcasted_iota(
        jnp.int32, (rows, rows), 1
    )

    def column_step(t):
        values = jnp.broadcast_to(pairs[t].astype(F32), (rows, rows))
        columns[t] = jnp.sum(jnp.where(same, values, 0.0), axis=1, keepdims=True)

    loop(0, groups, column_step)

    def image_step(step):
        score(me, arrive(0, image, step))

    lane = lax.broadcasted_iota(jnp.int32, (rows, rows), 1)

    def hits(t, i):
        return columns[t] == (lane + i * rows).astype(F32)

    def over(count, first, join, value):
        if count <= 8:
            total = first
            for number in range(count):
                total = join(total, value(number))
            return total
        return lax.fori_loop(0, count, lambda n, total: join(total, value(n)), first)

    add = lambda left, right: left + right
    low = -jnp.inf

    def row_step(t):
        top = over(
            groups,
            jnp.full((rows, 1), low, F32),
            jnp.maximum,
            lambda i: jnp.max(scores[t, i], axis=1, keepdims=True),
        )

        def term(i):
            value = jnp.exp(scores[t, i] - top)
            row_exp[t, i] = value
            return jnp.sum(value, axis=1, keepdims=True)

        amount = over(groups, jnp.zeros((rows, 1), F32), add, term)
        row_scale[t] = 1.0 / amount
        hit_sum = over(
            groups,
            jnp.zeros((1, rows), F32),
            add,
            lambda i: jnp.sum(jnp.where(hits(t, i), scores[t, i], 0.0), axis=0, keepdims=True),
        )
        terms[t] = (
            jnp.sum(top + jnp.log(amount), keepdims=True)
            - 2.0 * jnp.sum(hit_sum, axis=1, keepdims=True)
        )

    def col_step(i, total):
        top = over(
            groups,
            jnp.full((1, rows), low, F32),
            jnp.maximum,
            lambda t: jnp.max(scores[t, i], axis=0, keepdims=True),
        )

        def term(t):
            value = jnp.exp(scores[t, i] - top)
            col_exp[t, i] = value
            return jnp.sum(value, axis=0, keepdims=True)

        amount = over(groups, jnp.zeros((1, rows), F32), add, term)
        col_scale[i] = 1.0 / amount
        return total + jnp.sum(top + jnp.log(amount), axis=1, keepdims=True)

    def text_step(step):
        t = arrive(1, text, step)
        loop(0, groups, lambda i: score(t, i))
        row_step(t)

    loop(1, groups, image_step)
    row_step(me)
    loop(1, groups, text_step)
    total = jnp.zeros((1, 1), F32)
    for number in range(groups):
        total = col_step(number, total + terms[number])
    parts[blk] = jnp.broadcast_to(total, (1, 128))

    def tell(step, peer):
        return pltpu.make_async_remote_copy(
            src_ref=parts.at[blk],
            dst_ref=parts.at[blk],
            send_sem=loss_send.at[step, peer],
            recv_sem=loss_recv.at[step],
            device_id={"blk": lax.rem(blk + step, blocks), "grp": peer},
            device_id_type=MESH,
        )

    def hear(step):
        source = lax.rem(blk - step + blocks, blocks)
        pltpu.make_async_remote_copy(
            src_ref=parts.at[source],
            dst_ref=parts.at[source],
            send_sem=loss_send.at[step, 0],
            recv_sem=loss_recv.at[step],
            device_id={"blk": source, "grp": 0},
            device_id_type=MESH,
        ).wait_recv()

    @pl.when(sender)
    def _():
        pl.semaphore_wait(barrier, (blocks - 1) * groups)
        loop(1, blocks, lambda step: loop(0, groups, lambda peer: tell(step, peer).start()))

    def weight(t, i):
        return (
            row_exp[t, i] * row_scale[t]
            + col_exp[t, i] * col_scale[i]
            - jnp.where(hits(t, i), 2.0, 0.0)
        ).astype(jnp.bfloat16)

    half = score_scale * 0.5
    grad = jnp.zeros((rows, text_in.shape[2]), F32)
    out_text[...] = (
        over(
            groups,
            grad,
            add,
            lambda i: jnp.dot(weight(me, i), image[i], preferred_element_type=F32),
        )
        * half
    )
    store_text = pltpu.make_async_copy(out_text, grad_text.at[0], store_sem.at[0])
    store_text.start()
    out_image[...] = (
        over(
            groups,
            grad,
            add,
            lambda t: lax.dot_general(
                weight(t, me), text[t], (((0,), (0,)), ((), ())), preferred_element_type=F32
            ),
        )
        * half
    )
    store_image = pltpu.make_async_copy(out_image, grad_image.at[0], store_sem.at[1])
    store_image.start()

    for kind, buffer in enumerate(buffers):
        for piece in range(len(loads[kind])):
            loop(
                1,
                groups,
                lambda step, kind=kind, buffer=buffer, piece=piece: send(
                    kind, buffer, step, piece
                ).wait_send(),
            )

    @pl.when(sender)
    def _():
        loop(1, blocks, lambda step: loop(0, groups, lambda peer: tell(step, peer).wait_send()))

    loop(1, blocks, hear)
    everything = jnp.sum(parts[...].reshape(blocks, 128), axis=0, keepdims=True)
    loss[...] = everything[:, 0:1] / (2.0 * rows * groups * blocks)
    store_text.wait()
    store_image.wait()


def deliver(text_from, image_from, text_to, image_to, sem):
    half = text_from.shape[1] // 2
    copies = [
        pltpu.make_async_copy(
            source.at[0, pl.ds(part * half, half)],
            target.at[0, pl.ds(part * half, half)],
            sem.at[kind, part],
        )
        for part in range(2)
        for kind, (source, target) in enumerate(((text_from, text_to), (image_from, image_to)))
    ]
    for copy in copies:
        copy.start()
    for copy in copies:
        copy.wait()


def solution(mesh):
    groups, blocks = mesh.shape["grp"], mesh.shape["blk"]

    def local(text, image, pair_index):
        _, rows, width = text.shape
        anywhere = pl.BlockSpec(memory_space=pl.ANY)
        square = pltpu.VMEM((groups, groups, rows, rows), F32)
        grads_t, grads_i, loss = pl.pallas_call(
            functools.partial(kernel, groups, blocks),
            out_shape=(
                jax.ShapeDtypeStruct(text.shape, F32),
                jax.ShapeDtypeStruct(image.shape, F32),
                jax.ShapeDtypeStruct((1, 1), F32),
            ),
            in_specs=[pl.BlockSpec(memory_space=pltpu.HBM)] * 3,
            out_specs=(anywhere, anywhere, pl.BlockSpec(memory_space=pltpu.VMEM)),
            scratch_shapes=[
                pltpu.VMEM((groups, rows, width), text.dtype),
                pltpu.VMEM((groups, rows, width), image.dtype),
                pltpu.VMEM((groups, 1, rows), jnp.int32),
                square,
                square,
                square,
                pltpu.VMEM((groups, rows, 1), F32),
                pltpu.VMEM((groups, 1, rows), F32),
                pltpu.VMEM((groups, rows, 1), F32),
                pltpu.VMEM((blocks, 1, 128), F32),
                pltpu.VMEM((rows, width), F32),
                pltpu.VMEM((rows, width), F32),
                pltpu.SemaphoreType.DMA((3, 4)),
                pltpu.SemaphoreType.DMA((3, groups, 4)),
                pltpu.SemaphoreType.DMA((3, groups, 4)),
                pltpu.SemaphoreType.DMA((blocks, groups)),
                pltpu.SemaphoreType.DMA((blocks,)),
                pltpu.SemaphoreType.DMA((2,)),
                pltpu.SemaphoreType.REGULAR,
                pltpu.VMEM((groups, 1, 1), F32),
            ],
            compiler_params=pltpu.CompilerParams(collective_id=0, has_side_effects=True, vmem_limit_bytes=40 << 20),
        )(*(pltpu.with_memory_space_constraint(x, pltpu.HBM) for x in (text, image, pair_index)))
        grads_t, grads_i = pl.pallas_call(
            deliver,
            out_shape=(
                jax.ShapeDtypeStruct(text.shape, F32),
                jax.ShapeDtypeStruct(image.shape, F32),
            ),
            in_specs=[anywhere] * 2,
            out_specs=(pl.BlockSpec(memory_space=pltpu.HBM),) * 2,
            scratch_shapes=[pltpu.SemaphoreType.DMA((2, 2))],
            compiler_params=pltpu.CompilerParams(vmem_limit_bytes=1 << 20),
        )(grads_t, grads_i)
        return grads_t, grads_i, loss.reshape(())

    placed = (P("blk", "grp", None), P("blk", "grp", None), P("blk", "grp"))
    return jax.shard_map(
        local,
        mesh=mesh,
        in_specs=placed,
        out_specs=(P("blk", "grp", None), P("blk", "grp", None), P()),
        check_vma=False,
    )
```

```python
import functools

import jax
import jax.numpy as jnp
from jax import lax
from jax.experimental import pallas as pl
from jax.experimental.pallas import tpu as pltpu
from jax.sharding import PartitionSpec as P

score_scale = 0.125
MESH = pl.DeviceIdType.MESH
F32 = jnp.float32


def loop(start, stop, body):
    if stop - start <= 16:
        for number in range(start, stop):
            body(number)
    else:
        pl.loop(start, stop)(body)


def kernel(
    groups,
    blocks,
    text_in,
    image_in,
    pairs_in,
    grad_text,
    grad_image,
    parts,
    text,
    image,
    pairs,
    scores,
    row_exp,
    col_exp,
    row_scale,
    col_scale,
    columns,
    mine,
    out_text,
    out_image,
    load_sem,
    send_sem,
    recv_sem,
    loss_send,
    loss_recv,
    store_sem,
    ready,
):
    blk = lax.axis_index("blk")
    me = lax.axis_index("grp")
    rows = text_in.shape[1]

    loads = [
        pltpu.make_async_copy(source.at[0], target.at[me], load_sem.at[number])
        for number, (source, target) in enumerate(((image_in, image), (text_in, text)))
    ]
    loads.append(pltpu.make_async_copy(pairs_in, pairs.at[me], load_sem.at[2]))
    for load in loads:
        load.start()

    barrier = pltpu.get_barrier_semaphore()
    sender = me == 0

    def greet_group(peer):
        pl.semaphore_signal(barrier, inc=1, device_id={"grp": peer}, device_id_type=MESH)

    def greet_block(step):
        pl.semaphore_signal(
            barrier,
            inc=1,
            device_id={"blk": lax.rem(blk + step, blocks), "grp": 0},
            device_id_type=MESH,
        )

    @pl.when(sender)
    def _():
        loop(1, groups, greet_group)

    @pl.when(jnp.logical_not(sender))
    def _():
        pl.semaphore_wait(barrier, 1)
        pl.semaphore_signal(ready, inc=1, device_id={"grp": 0}, device_id_type=MESH)

    loop(1, blocks, greet_block)

    @pl.when(sender)
    def _():
        pl.semaphore_wait(ready, groups - 1)
        if groups > 2:

            def allow(peer):
                pl.semaphore_signal(ready, inc=1, device_id={"grp": peer}, device_id_type=MESH)

            loop(1, groups, allow)

    if groups > 2:

        @pl.when(jnp.logical_not(sender))
        def _():
            pl.semaphore_wait(ready, 1)

    def send(kind, buffer, step):
        peer = lax.rem(me + step, groups)
        return pltpu.make_async_remote_copy(
            src_ref=(image_in.at[0], text_in.at[0], pairs_in)[kind],
            dst_ref=buffer.at[me],
            send_sem=send_sem.at[kind, step],
            recv_sem=recv_sem.at[kind, step],
            device_id={"grp": peer},
            device_id_type=MESH,
        )

    def arrive(kind, buffer, step):
        source = lax.rem(me - step + groups, groups)
        pltpu.make_async_remote_copy(
            src_ref=buffer.at[source],
            dst_ref=buffer.at[source],
            send_sem=send_sem.at[kind, step],
            recv_sem=recv_sem.at[kind, step],
            device_id={"grp": source},
            device_id_type=MESH,
        ).wait_recv()
        return source

    buffers = (image, text, pairs)
    for kind, buffer in ((2, pairs), (0, image), (1, text)):
        loop(1, groups, lambda step, kind=kind, buffer=buffer: send(kind, buffer, step).start())
    for load in loads:
        load.wait()

    def score(t, i):
        scores[t, i] = (
            lax.dot_general(
                text[t], image[i], (((1,), (1,)), ((), ())), preferred_element_type=F32
            )
            * score_scale
        )

    score(me, me)

    def pair_step(step):
        arrive(2, pairs, step)

    loop(1, groups, pair_step)
    same = lax.broadcasted_iota(jnp.int32, (rows, rows), 0) == lax.broadcasted_iota(
        jnp.int32, (rows, rows), 1
    )

    def column_step(t):
        values = jnp.broadcast_to(pairs[t].astype(F32), (rows, rows))
        columns[t] = jnp.sum(jnp.where(same, values, 0.0), axis=1, keepdims=True)

    loop(0, groups, column_step)

    def image_step(step):
        score(me, arrive(0, image, step))

    def text_step(step):
        t = arrive(1, text, step)
        loop(0, groups, lambda i: score(t, i))

    loop(1, groups, image_step)
    loop(1, groups, text_step)

    lane = lax.broadcasted_iota(jnp.int32, (rows, rows), 1)

    def hits(t, i):
        return columns[t] == (lane + i * rows).astype(F32)

    def over(count, first, join, value):
        if count <= 8:
            total = first
            for number in range(count):
                total = join(total, value(number))
            return total
        return lax.fori_loop(0, count, lambda n, total: join(total, value(n)), first)

    add = lambda left, right: left + right
    low = -jnp.inf

    def row_step(t, total):
        top = over(
            groups,
            jnp.full((rows, 1), low, F32),
            jnp.maximum,
            lambda i: jnp.max(scores[t, i], axis=1, keepdims=True),
        )

        def term(i):
            value = jnp.exp(scores[t, i] - top)
            row_exp[t, i] = value
            return jnp.sum(value, axis=1, keepdims=True)

        amount = over(groups, jnp.zeros((rows, 1), F32), add, term)
        row_scale[t] = 1.0 / amount
        hit_sum = over(
            groups,
            jnp.zeros((1, rows), F32),
            add,
            lambda i: jnp.sum(jnp.where(hits(t, i), scores[t, i], 0.0), axis=0, keepdims=True),
        )
        return (
            total
            + jnp.sum(top + jnp.log(amount), keepdims=True)
            - 2.0 * jnp.sum(hit_sum, axis=1, keepdims=True)
        )

    def col_step(i, total):
        top = over(
            groups,
            jnp.full((1, rows), low, F32),
            jnp.maximum,
            lambda t: jnp.max(scores[t, i], axis=0, keepdims=True),
        )

        def term(t):
            value = jnp.exp(scores[t, i] - top)
            col_exp[t, i] = value
            return jnp.sum(value, axis=0, keepdims=True)

        amount = over(groups, jnp.zeros((1, rows), F32), add, term)
        col_scale[i] = 1.0 / amount
        return total + jnp.sum(top + jnp.log(amount), axis=1, keepdims=True)

    total = jnp.zeros((1, 1), F32)
    for number in range(groups):
        total = row_step(number, total)
    for number in range(groups):
        total = col_step(number, total)
    mine[...] = jnp.broadcast_to(total, (1, 128))

    def tell(step, peer):
        return pltpu.make_async_remote_copy(
            src_ref=mine,
            dst_ref=parts.at[blk],
            send_sem=loss_send.at[step, peer],
            recv_sem=loss_recv.at[step],
            device_id={"blk": lax.rem(blk + step, blocks), "grp": peer},
            device_id_type=MESH,
        )

    def hear(step):
        source = lax.rem(blk - step + blocks, blocks)
        pltpu.make_async_remote_copy(
            src_ref=parts.at[source],
            dst_ref=parts.at[source],
            send_sem=loss_send.at[step, 0],
            recv_sem=loss_recv.at[step],
            device_id={"blk": source, "grp": 0},
            device_id_type=MESH,
        ).wait_recv()

    @pl.when(sender)
    def _():
        pl.semaphore_wait(barrier, (blocks - 1) * groups)
        loop(1, blocks, lambda step: loop(0, groups, lambda peer: tell(step, peer).start()))

    keep = pltpu.make_async_copy(mine, parts.at[blk], store_sem.at[2])
    keep.start()

    def weight(t, i):
        return (
            row_exp[t, i] * row_scale[t]
            + col_exp[t, i] * col_scale[i]
            - jnp.where(hits(t, i), 2.0, 0.0)
        ).astype(jnp.bfloat16)

    half = score_scale * 0.5
    grad = jnp.zeros((rows, text_in.shape[2]), F32)
    out_text[...] = (
        over(
            groups,
            grad,
            add,
            lambda i: jnp.dot(weight(me, i), image[i], preferred_element_type=F32),
        )
        * half
    )
    store_text = pltpu.make_async_copy(out_text, grad_text.at[0], store_sem.at[0])
    store_text.start()
    out_image[...] = (
        over(
            groups,
            grad,
            add,
            lambda t: lax.dot_general(
                weight(t, me), text[t], (((0,), (0,)), ((), ())), preferred_element_type=F32
            ),
        )
        * half
    )
    store_image = pltpu.make_async_copy(out_image, grad_image.at[0], store_sem.at[1])
    store_image.start()

    for kind, buffer in enumerate(buffers):
        loop(
            1, groups, lambda step, kind=kind, buffer=buffer: send(kind, buffer, step).wait_send()
        )

    @pl.when(sender)
    def _():
        loop(1, blocks, lambda step: loop(0, groups, lambda peer: tell(step, peer).wait_send()))

    loop(1, blocks, hear)
    keep.wait()
    store_text.wait()
    store_image.wait()


def deliver(
    pairs_total, text_from, image_from, parts_from, text_to, image_to, loss_to, parts, loss, sem
):
    half = text_from.shape[1] // 2
    copies = [
        pltpu.make_async_copy(
            source.at[0, pl.ds(part * half, half)],
            target.at[0, pl.ds(part * half, half)],
            sem.at[kind, part],
        )
        for part in range(2)
        for kind, (source, target) in enumerate(((text_from, text_to), (image_from, image_to)))
    ]
    fetch = pltpu.make_async_copy(parts_from, parts, sem.at[2, 0])
    fetch.start()
    for copy in copies:
        copy.start()
    fetch.wait()
    total = jnp.sum(parts[...].reshape(parts.shape[0], 128), axis=0, keepdims=True)
    loss[...] = total[:, 0:1] / (2.0 * pairs_total)
    put = pltpu.make_async_copy(loss, loss_to, sem.at[2, 1])
    put.start()
    for copy in copies:
        copy.wait()
    put.wait()


def solution(mesh):
    groups, blocks = mesh.shape["grp"], mesh.shape["blk"]

    def local(text, image, pair_index):
        _, rows, width = text.shape
        anywhere = pl.BlockSpec(memory_space=pl.ANY)
        square = pltpu.VMEM((groups, groups, rows, rows), F32)
        grads_t, grads_i, parts = pl.pallas_call(
            functools.partial(kernel, groups, blocks),
            out_shape=(
                jax.ShapeDtypeStruct(text.shape, F32),
                jax.ShapeDtypeStruct(image.shape, F32),
                jax.ShapeDtypeStruct((blocks, 1, 128), F32),
            ),
            in_specs=[pl.BlockSpec(memory_space=pltpu.HBM)] * 3,
            out_specs=(anywhere,) * 3,
            scratch_shapes=[
                pltpu.VMEM((groups, rows, width), text.dtype),
                pltpu.VMEM((groups, rows, width), image.dtype),
                pltpu.VMEM((groups, 1, rows), jnp.int32),
                square,
                square,
                square,
                pltpu.VMEM((groups, rows, 1), F32),
                pltpu.VMEM((groups, 1, rows), F32),
                pltpu.VMEM((groups, rows, 1), F32),
                pltpu.VMEM((1, 128), F32),
                pltpu.VMEM((rows, width), F32),
                pltpu.VMEM((rows, width), F32),
                pltpu.SemaphoreType.DMA((3,)),
                pltpu.SemaphoreType.DMA((3, groups)),
                pltpu.SemaphoreType.DMA((3, groups)),
                pltpu.SemaphoreType.DMA((blocks, groups)),
                pltpu.SemaphoreType.DMA((blocks,)),
                pltpu.SemaphoreType.DMA((3,)),
                pltpu.SemaphoreType.REGULAR,
            ],
            compiler_params=pltpu.CompilerParams(collective_id=0, has_side_effects=True, vmem_limit_bytes=40 << 20),
        )(*(pltpu.with_memory_space_constraint(x, pltpu.HBM) for x in (text, image, pair_index)))
        grads_t, grads_i, loss = pl.pallas_call(
            functools.partial(deliver, rows * groups * blocks),
            out_shape=(
                jax.ShapeDtypeStruct(text.shape, F32),
                jax.ShapeDtypeStruct(image.shape, F32),
                jax.ShapeDtypeStruct((1, 1), F32),
            ),
            in_specs=[anywhere] * 3,
            out_specs=(pl.BlockSpec(memory_space=pltpu.HBM),) * 3,
            scratch_shapes=[
                pltpu.VMEM((blocks, 1, 128), F32),
                pltpu.VMEM((1, 1), F32),
                pltpu.SemaphoreType.DMA((3, 2)),
            ],
            compiler_params=pltpu.CompilerParams(vmem_limit_bytes=1 << 20),
        )(grads_t, grads_i, parts)
        return grads_t, grads_i, loss.reshape(())

    placed = (P("blk", "grp", None), P("blk", "grp", None), P("blk", "grp"))
    return jax.shard_map(
        local,
        mesh=mesh,
        in_specs=placed,
        out_specs=(P("blk", "grp", None), P("blk", "grp", None), P()),
        check_vma=False,
    )
```
